32 devices in a mesh: dp: 2 (over x), expert: 4 (over z), tensor: 4 (over y, core).
Axes of the slice: x: 2, y: 2, z: 4, core: 2. Of those that a mesh axis runs over, the one named last changes fastest.
Arguments:
- tokens: bfloat16 [1024, 7168], P(('dp', 'expert'), 'tensor'), may hold values from -6 to 6
- expert_ids: int32 [1024, 2], P(('dp', 'expert')), may hold values from 0 to 3, all different within a row; in each aligned block of 128 rows (0 to 127, 128 to 255, ...) at most 96 rows name the same one
- gate_scores: bfloat16 [1024, 2], P(('dp', 'expert')), may hold values from 0.099609375 to 0.59765625
- weight_in: bfloat16 [4, 2, 7168, 1024], P('expert', None, 'tensor', 'dp'), may hold values from -0.0625 to 0.0625
- weight_out: bfloat16 [4, 1024, 7168], P('expert', 'dp', 'tensor'), may hold values from -0.1875 to 0.1875
Outputs:
- mixed: bfloat16 [1024, 7168], P(('dp', 'expert'), 'tensor')
The draws below stay inside these ranges and needn't reach their ends.
Inputs may be any that keep to these rules, and one draw needn't show every extreme that they name: `expert_ids`: each token names 2 different experts; among the 128 tokens of one index of dp and expert together (aligned blocks of rows) no expert is named more than 96 times, and in some blocks an expert is named exactly 96 times.
All inputs are finite; a program needn't handle non-finite values.
Results may differ from the reference program's by a relative error of at most 0.0071.
Values may be sent and summed in bfloat16 or wider, within the bound.
A program may use at most 64 MiB of HBM per device.

```python
import math
import jax
import jax.numpy as jnp
import numpy as np
from jax import lax

D = 7168
FF = 1024
TOK_GRP = 128
TOP = 2
EXPERTS = 4
CAP = 96
TOKENS = 1024


def shard_levels(rng, dims, cuts, low, top_value):
    level = 1.0
    for position, shards_of in cuts:
        heights = jax.random.uniform(jax.random.fold_in(jax.random.fold_in(rng, 6), position), (shards_of,), jnp.float32, low / len(cuts), top_value / len(cuts))
        level = level * jnp.repeat(jnp.exp(heights), dims[position] // shards_of).reshape((-1,) + (1,) * (len(dims) - 1 - position))
    return level


def routed_block(own_key, own, number, rows, count, top, limit, lean):
    order = jax.random.permutation(own_key, count)
    crowded, usual = shares(count, rows * top, limit, lean, True), shares(count, rows * top, limit, lean, False)
    places = jnp.arange(count)

    def named(tallies, offset_by):
        used = int((tallies > 0).sum())
        fixed = max(1, used // 4)
        shifted = fixed + (places - fixed + offset_by * (used - fixed)) % max(1, count - fixed)
        return jnp.zeros((count,), jnp.int32).at[order[jnp.where(places < fixed, places, shifted)]].set(jnp.asarray(tallies, jnp.int32))

    tallies = jnp.where(number % 4 == 0, named(crowded, number // 4), named(usual, number - number // 4 - 1))
    mixed = jax.random.permutation(jax.random.fold_in(own, 3), count)
    giver, sink = mixed[0:count // 2 * 2:2], mixed[1:count // 2 * 2:2]
    slack = jnp.minimum(tallies[giver] - 1, limit - tallies[sink]) // 2
    slack = jnp.where((giver == order[0]) | (sink == order[0]) | (tallies[sink] == 0), 0, jnp.maximum(slack, 0))
    shifted = jax.random.randint(jax.random.fold_in(own, 4), (count // 2,), 0, 1 << 20) % (slack + 1)
    tallies = tallies.at[giver].add(-shifted).at[sink].add(shifted)
    members = jnp.searchsorted(jnp.cumsum(tallies), jnp.arange(rows * top), side="right").astype(jnp.int32)
    table = members.reshape(top, rows).T
    table = table[jax.random.permutation(jax.random.fold_in(own, 1), rows)]
    offset_by = jax.random.randint(jax.random.fold_in(own, 2), (rows, 1), 0, top)
    return jnp.take_along_axis(table, (jnp.arange(top)[None, :] + offset_by) % top, axis=1)


def shares(count, total, most, slope, full):
    portions = [(1 << 20) // math.isqrt(rank ** slope) + 1 for rank in range(1, count + 1)]
    largest = most if full else min(most, max(-(-total // count), total * portions[0] // sum(portions)))
    least = 1 if total - largest >= count - 1 else 0
    holding, spare = [largest] + [least] * (count - 1), total - largest - least * (count - 1)
    while spare > 0:
        movable = [i for i in range(1, count) if holding[i] < largest] or [i for i in range(1, count) if holding[i] < most]
        whole, budget = sum([portions[i] for i in movable]), spare
        for i in movable:
            more = min(most - holding[i], max(1, budget * portions[i] // whole), spare)
            holding[i] = holding[i] + more
            spare = spare - more
    return np.array(holding)


def noise(own_key, shape, width, limit, cuts=(), kind=jnp.bfloat16):
    drawn = width * jax.random.normal(own_key, shape, jnp.float32)
    if cuts:
        drawn = drawn * shard_levels(own_key, shape, cuts, -0.22, 0.18)
    return jnp.clip(drawn, -limit, limit).astype(kind)


def setup_inputs(seed: int = 0) -> dict:
    key_list = jax.random.split(jax.random.key(seed), 6)
    tokens = noise(key_list[0], (TOKENS, D), 1.0, 6.0, ((0, 8), (1, 4)))
    expert_ids_keys = jax.random.split(jax.random.fold_in(key_list[1], 1), TOKENS // TOK_GRP)
    expert_ids_turns = jax.random.permutation(jax.random.fold_in(key_list[1], 3), TOKENS // TOK_GRP)
    expert_ids = jax.vmap(lambda own, number: routed_block(jax.random.fold_in(key_list[1], 2), own, number, TOK_GRP, EXPERTS, TOP, CAP, 1))(expert_ids_keys, expert_ids_turns).reshape((TOKENS, TOP))
    gate_scores = jnp.clip(0.099609375 + 0.49804688 * jax.random.uniform(key_list[2], (TOKENS, TOP), jnp.float32) ** shard_levels(key_list[2], (TOKENS, TOP), ((0, 8),), -0.2, 0.2), 0.099609375, 0.59765625).astype(jnp.bfloat16)
    weight_in = noise(key_list[3], (EXPERTS, 2, D, FF), D ** -0.5, 0.0625, ((0, 4), (2, 4), (3, 2)))
    weight_out = noise(key_list[4], (EXPERTS, FF, D), FF ** -0.5, 0.1875, ((0, 4), (1, 2), (2, 4)))
    return dict(tokens=tokens, expert_ids=expert_ids, gate_scores=gate_scores, weight_in=weight_in, weight_out=weight_out)


def reference(tokens, expert_ids, gate_scores, weight_in, weight_out):
    groups = TOKENS // TOK_GRP
    wide = tokens.astype(jnp.float32)
    mean_square = lax.optimization_barrier(jnp.mean(wide * wide, axis=1, keepdims=True))
    normed = (wide * lax.rsqrt(mean_square + 1e-06)).astype(jnp.bfloat16)
    grouped = normed.reshape(groups, TOK_GRP, D).astype(jnp.float32)
    flat_ids = expert_ids.reshape(groups, TOK_GRP * TOP)
    one_hot = (flat_ids[:, :, None] == jnp.arange(EXPERTS, dtype=jnp.int32)[None, None, :]).astype(jnp.int32)
    earlier = jnp.cumsum(one_hot, axis=1) - one_hot
    slot_pos = lax.optimization_barrier(jnp.sum(earlier * one_hot, axis=2)).astype(jnp.int32)
    slot_range = jnp.arange(CAP, dtype=jnp.int32)
    scores = gate_scores.astype(jnp.float32).reshape(groups, TOK_GRP, TOP, 1)

    def one_expert(totals, inputs):
        expert, gate_up, down = inputs
        matched = (flat_ids == expert)[:, :, None] & (slot_pos[:, :, None] == slot_range[None, None, :])
        matched = matched.astype(jnp.float32).reshape(groups, TOK_GRP, TOP, CAP)
        picked = lax.optimization_barrier(jnp.sum(matched, axis=2))
        gathered = jnp.einsum('gtc,gtd->gcd', picked, grouped).astype(jnp.bfloat16).reshape(groups * CAP, D)
        gate = jnp.dot(gathered, gate_up[0], preferred_element_type=jnp.float32)
        upward = jnp.dot(gathered, gate_up[1], preferred_element_type=jnp.float32)
        hidden = (jax.nn.silu(gate) * upward).astype(jnp.bfloat16)
        result = jnp.dot(hidden, down, preferred_element_type=jnp.float32).astype(jnp.bfloat16)
        result = result.reshape(groups, CAP, D).astype(jnp.float32)
        weights = lax.optimization_barrier(jnp.sum(matched * scores, axis=2))
        return (totals + jnp.einsum('gtc,gcd->gtd', weights, result), None)
    start_total = jnp.zeros((groups, TOK_GRP, D), jnp.float32)
    totals, unused = lax.scan(one_expert, start_total, (jnp.arange(EXPERTS, dtype=jnp.int32), weight_in, weight_out))
    return totals.reshape(TOKENS, D).astype(jnp.bfloat16)
```

```python
import functools

import jax
import jax.numpy as jnp
from jax import lax
from jax.experimental import pallas as pl
from jax.experimental.pallas import tpu as pltpu
from jax.sharding import PartitionSpec as P

MESH = pl.DeviceIdType.MESH
F32 = jnp.float32
BF16 = jnp.bfloat16


def dot(a, b):
    return jnp.dot(a, b, preferred_element_type=F32)


def kernel(
    sizes,
    tokens,
    ids,
    ids_t,
    scores,
    w_in_hbm,
    w_out_hbm,
    mixed,
    w_in,
    w_out,
    slot_t,
    combine,
    outgoing,
    rows_in,
    part,
    part_in,
    hidden,
    down,
    down_in,
    home,
    home_in,
    w_sem,
    sz,
    rz,
    sx,
    rx,
    sp,
    rp,
    sh,
    rh,
    so,
    ro,
    sr,
    rr,
):
    n_dp, n_ex, n_t, cap = sizes
    d, e, t = lax.axis_index("dp"), lax.axis_index("expert"), lax.axis_index("tensor")
    group = n_ex // n_t
    ec = e // group
    tok, width = tokens.shape
    top = ids.shape[1]
    units = w_out.shape[0]
    width_all = width * n_t
    chunk_rows = group * cap

    def at(index, step, count):
        return lax.rem(index + step + count, count)

    def copy(src, dst, send, recv, axis, index):
        return pltpu.make_async_remote_copy(
            src_ref=src, dst_ref=dst, send_sem=send, recv_sem=recv,
            device_id={axis: index}, device_id_type=MESH,
        )

    barrier = pltpu.get_barrier_semaphore()
    for axis, me, count in (("dp", d, n_dp), ("expert", e, n_ex), ("tensor", t, n_t)):
        for step in range(1, count):
            pl.semaphore_signal(
                barrier, inc=1, device_id={axis: at(me, step, count)}, device_id_type=MESH
            )
    load_in = pltpu.make_async_copy(w_in_hbm.at[0], w_in, w_sem.at[0])
    load_out = pltpu.make_async_copy(w_out_hbm.at[0], w_out, w_sem.at[1])
    load_in.start()
    load_out.start()

    wide_ex = max(128, n_ex)
    ex_rows = lax.broadcasted_iota(jnp.int32, (wide_ex, tok), 0)
    named_t = ex_rows == ids_t[0:1, :]
    for k in range(1, top):
        named_t = named_t | (ex_rows == ids_t[k : k + 1, :])
    before = lax.broadcasted_iota(jnp.int32, (tok, tok), 0) < lax.broadcasted_iota(
        jnp.int32, (tok, tok), 1
    )
    count_t = dot(named_t.astype(F32).astype(BF16), before.astype(F32).astype(BF16))
    slot_t[...] = jnp.where(named_t, count_t, -1.0)
    slot_rows = lax.broadcasted_iota(jnp.int32, (cap, tok), 0).astype(F32)

    def picked(expert):
        pick = (slot_rows == slot_t[pl.ds(expert, 1), :]).astype(F32).astype(BF16)
        return dot(pick, tokens[...]).astype(BF16)

    def block(ref, lead, expert):
        if group == 1:
            return ref.at[lead, expert]
        return ref.at[lead, expert // group, pl.ds(pl.multiple_of(lax.rem(expert, group) * cap, cap), cap)]

    def send_z(expert):
        return copy(outgoing.at[expert], block(rows_in, 0, e), sz.at[expert], rz.at[e], "expert", expert)

    def wait_z(source):
        return copy(outgoing.at[source], block(rows_in, 0, source), sz.at[source], rz.at[source], "expert", source)

    pl.semaphore_wait(barrier, n_dp + n_ex + n_t - 3)

    outgoing[e] = picked(e)
    own = pltpu.make_async_copy(outgoing.at[e], block(rows_in, 0, e), w_sem.at[2])
    own.start()

    def forward_x(expert, step):
        return copy(
            block(rows_in, 0, expert), block(rows_in, n_dp - step, expert),
            sx.at[step, expert], rx.at[n_dp - step, expert], "dp", at(d, step, n_dp),
        )

    def wait_x(expert, h):
        return copy(
            block(rows_in, 0, expert), block(rows_in, h, expert),
            sx.at[h, expert], rx.at[h, expert], "dp", at(d, h, n_dp),
        )

    @pl.loop(1, n_ex)
    def _(step):
        expert = at(e, step, n_ex)
        outgoing[expert] = picked(expert)
        send_z(expert).start()

    own.wait()

    ex_lanes = lax.broadcasted_iota(jnp.int32, (tok, wide_ex), 1)
    named = ex_lanes == ids[:, 0:1]
    for k in range(1, top):
        named = named | (ex_lanes == ids[:, k : k + 1])
    after = lax.broadcasted_iota(jnp.int32, (tok, tok), 1) < lax.broadcasted_iota(
        jnp.int32, (tok, tok), 0
    )
    counts = dot(after.astype(F32).astype(BF16), named.astype(F32).astype(BF16))
    lanes = lax.broadcasted_iota(jnp.int32, (tok, n_ex * cap), 1).astype(F32)
    weights = jnp.zeros((tok, n_ex * cap), F32)
    for k in range(top):
        this = ids[:, k : k + 1]
        slot = jnp.sum(jnp.where(ex_lanes == this, counts, 0.0), axis=1, keepdims=True)
        target = this.astype(F32) * cap + slot
        weights = weights + jnp.where(lanes == target, scores[:, k : k + 1].astype(F32), 0.0)
    combine[...] = weights.astype(BF16)

    load_in.wait()

    def part_copy(h, c):
        return copy(part.at[h, c], part_in.at[h, t], sp.at[h, c], rp.at[h, t], "tensor", c)

    def project(h, c):
        rows = rows_in[h, c]
        for g in range(2):
            part[h, c, :, g * units : (g + 1) * units] = dot(rows, w_in[g]).astype(BF16)
        wide = rows.astype(F32)
        squares = jnp.sum(wide * wide, axis=1, keepdims=True)
        high = squares.astype(BF16).astype(F32)
        lane = lax.broadcasted_iota(jnp.int32, (chunk_rows, 128), 1)
        part[h, c, :, 2 * units :] = jnp.where(lane < 64, high, squares - high).astype(BF16)

        @pl.when(c != t)
        def _():
            part_copy(h, c).start()

    @pl.loop(0, n_t + 1)
    def _(step):
        @pl.when(step < n_t)
        def _():
            c = at(ec, -step, n_t)
            for i in range(group):
                source = c * group + i

                @pl.when(source != e)
                def _():
                    wait_z(source).wait_recv()

                for hop in range(1, n_dp):
                    forward_x(source, hop).start()
            project(0, c)

        @pl.when(step > 0)
        def _():
            c = at(ec, 1 - step, n_t)
            for h in range(1, n_dp):
                for i in range(group):
                    wait_x(c * group + i, h).wait_recv()
                project(h, c)

    def hidden_copy(h, step):
        return copy(hidden.at[h, t], hidden.at[h, t], sh.at[h, step], rh.at[h, t], "tensor", at(t, step, n_t))

    for h in range(n_dp):
        total = part[h, t].astype(F32)
        for step in range(1, n_t):
            s = at(t, step, n_t)
            copy(part.at[h, s], part_in.at[h, s], sp.at[h, s], rp.at[h, s], "tensor", s).wait_recv()
            total = total + part_in[h, s].astype(F32)
        squares = total[:, 2 * units : 2 * units + 1] + total[:, 2 * units + 64 : 2 * units + 65]
        scale = lax.rsqrt(squares / width_all + 1e-06)
        gate = total[:, :units] * scale
        up = total[:, units : 2 * units] * scale
        hidden[h, t] = (gate / (1.0 + jnp.exp(-gate)) * up).astype(BF16)
        for step in range(1, n_t):
            hidden_copy(h, step).start()

    load_out.wait()

    def wait_hidden(h, q):
        @pl.when(q != t)
        def _():
            copy(hidden.at[h, q], hidden.at[h, q], sh.at[h, 0], rh.at[h, q], "tensor", q).wait_recv()

    def down_copy(h, q):
        return copy(down.at[h, q], down_in.at[n_dp - h, q], so.at[h, q], ro.at[n_dp - h, q], "dp", at(d, h, n_dp))

    @pl.loop(0, n_t)
    def _(step):
        q = at(ec, 1 + step, n_t)
        for h in range(1, n_dp):
            wait_hidden(h, q)
            down[h, q] = dot(hidden[h, q], w_out[...]).astype(BF16)
            down_copy(h, q).start()

    def home_copy(expert):
        return copy(block(home, 0, expert), home_in.at[e], sr.at[expert], rr.at[e], "expert", expert)

    @pl.loop(0, n_t)
    def _(step):
        q = at(ec, 1 + step, n_t)
        wait_hidden(0, q)
        total = dot(hidden[0, q], w_out[...])
        for h in range(1, n_dp):
            copy(down.at[h, q], down_in.at[h, q], so.at[h, q], ro.at[h, q], "dp", at(d, h, n_dp)).wait_recv()
            total = total + down_in[h, q].astype(F32)
        home[0, q] = total.astype(BF16)
        for i in range(group):
            expert = q * group + i

            @pl.when(expert != e)
            def _():
                home_copy(expert).start()

            @pl.when(expert == e)
            def _():
                home_in[expert] = home[0, q, i * cap : (i + 1) * cap, :]

    @pl.loop(1, n_ex)
    def _(step):
        source = at(e, step, n_ex)
        copy(block(home, 0, source), home_in.at[source], sr.at[source], rr.at[source], "expert", source).wait_recv()

    mixed[...] = dot(combine[...], home_in[...].reshape(n_ex * cap, width)).astype(BF16)

    @pl.loop(1, n_ex)
    def _(step):
        expert = at(e, step, n_ex)
        send_z(expert).wait_send()
        home_copy(expert).wait_send()

    @pl.loop(0, n_ex)
    def _(expert):
        for hop in range(1, n_dp):
            forward_x(expert, hop).wait_send()

    for h in range(n_dp):
        for step in range(1, n_t):
            part_copy(h, at(t, step, n_t)).wait_send()
            hidden_copy(h, step).wait_send()
    for h in range(1, n_dp):
        for q in range(n_t):
            down_copy(h, q).wait_send()


def per_device(sizes, tokens, expert_ids, gate_scores, weight_in, weight_out):
    n_dp, n_ex, n_t, cap = sizes
    tok, width = tokens.shape
    units = weight_out.shape[1]
    chunk = n_ex // n_t * cap
    dma = pltpu.SemaphoreType.DMA
    vmem = pl.BlockSpec(memory_space=pltpu.VMEM)
    return pl.pallas_call(
        functools.partial(kernel, sizes),
        out_shape=jax.ShapeDtypeStruct((tok, width), BF16),
        in_specs=[vmem] * 4 + [pl.BlockSpec(memory_space=pl.ANY)] * 2,
        out_specs=vmem,
        scratch_shapes=[
            pltpu.VMEM((2, width, units), BF16),
            pltpu.VMEM((units, width), BF16),
            pltpu.VMEM((max(128, n_ex), tok), F32),
            pltpu.VMEM((tok, n_ex * cap), BF16),
            pltpu.VMEM((n_ex, cap, width), BF16),
            pltpu.VMEM((n_dp, n_t, chunk, width), BF16),
            pltpu.VMEM((n_dp, n_t, chunk, 2 * units + 128), BF16),
            pltpu.VMEM((n_dp, n_t, chunk, 2 * units + 128), BF16),
            pltpu.VMEM((n_dp, n_t, chunk, units), BF16),
            pltpu.VMEM((n_dp, n_t, chunk, width), BF16),
            pltpu.VMEM((n_dp, n_t, chunk, width), BF16),
            pltpu.VMEM((1, n_t, chunk, width), BF16),
            pltpu.VMEM((n_ex, cap, width), BF16),
            dma((3,)),
            dma((n_ex,)),
            dma((n_ex,)),
            dma((n_dp, n_ex)),
            dma((n_dp, n_ex)),
            dma((n_dp, n_t)),
            dma((n_dp, n_t)),
            dma((n_dp, n_t)),
            dma((n_dp, n_t)),
            dma((n_dp, n_t)),
            dma((n_dp, n_t)),
            dma((n_ex,)),
            dma((n_ex,)),
        ],
        compiler_params=pltpu.CompilerParams(
            collective_id=0, has_side_effects=True, vmem_limit_bytes=60 * 1024 * 1024
        ),
    )(tokens, expert_ids, expert_ids.T, gate_scores, weight_in, weight_out)


def solution(mesh):
    n_dp, n_ex, n_t = mesh.shape["dp"], mesh.shape["expert"], mesh.shape["tensor"]

    def whole(tokens, expert_ids, gate_scores, weight_in, weight_out):
        tok = tokens.shape[0] // (n_dp * n_ex)
        slots = min(3 * tok * expert_ids.shape[1] // (2 * n_ex), tok)
        cap = -(-slots // 16) * 16
        return jax.shard_map(
            functools.partial(per_device, (n_dp, n_ex, n_t, cap)),
            mesh=mesh,
            in_specs=(
                P(("dp", "expert"), "tensor"),
                P(("dp", "expert"), None),
                P(("dp", "expert"), None),
                P("expert", None, "tensor", "dp"),
                P("expert", "dp", "tensor"),
            ),
            out_specs=P(("dp", "expert"), "tensor"),
            check_vma=False,
        )(tokens, expert_ids, gate_scores, weight_in, weight_out)

    return whole
```

```python
import functools

import jax
import jax.numpy as jnp
from jax import lax
from jax.experimental import pallas as pl
from jax.experimental.pallas import tpu as pltpu
from jax.sharding import PartitionSpec as P

MESH = pl.DeviceIdType.MESH
F32 = jnp.float32
BF16 = jnp.bfloat16


def dot(a, b):
    return jnp.dot(a, b, preferred_element_type=F32)


def kernel(
    sizes,
    tokens,
    ids,
    scores,
    w_in_hbm,
    w_out_hbm,
    mixed,
    w_in,
    w_out,
    squares,
    normed,
    slot_t,
    combine,
    outgoing,
    rows_in,
    part,
    part_in,
    hidden,
    keep,
    down,
    down_in,
    home,
    home_in,
    w_sem,
    sq,
    rq,
    sz,
    rz,
    sx,
    rx,
    sp,
    rp,
    sh,
    rh,
    so,
    ro,
    sr,
    rr,
):
    n_dp, n_ex, n_t, cap = sizes
    d, e, t = lax.axis_index("dp"), lax.axis_index("expert"), lax.axis_index("tensor")
    group = n_ex // n_t
    ec = e // group
    tok, width = tokens.shape
    top = ids.shape[1]
    units = w_out.shape[0]
    sub = units // n_t
    width_all = width * n_t

    def at(index, step, count):
        return lax.rem(index + step + count, count)

    def copy(src, dst, send, recv, axis, index):
        return pltpu.make_async_remote_copy(
            src_ref=src, dst_ref=dst, send_sem=send, recv_sem=recv,
            device_id={axis: index}, device_id_type=MESH,
        )

    barrier = pltpu.get_barrier_semaphore()
    for axis, me, count in (("dp", d, n_dp), ("expert", e, n_ex), ("tensor", t, n_t)):
        for step in range(1, count):
            pl.semaphore_signal(
                barrier, inc=1, device_id={axis: at(me, step, count)}, device_id_type=MESH
            )
    load_in = pltpu.make_async_copy(w_in_hbm.at[0], w_in, w_sem.at[0])
    load_out = pltpu.make_async_copy(w_out_hbm.at[0], w_out, w_sem.at[1])
    load_in.start()
    load_out.start()

    tok_rows = lax.broadcasted_iota(jnp.int32, (tok, tok), 0)
    tok_lanes = lax.broadcasted_iota(jnp.int32, (tok, tok), 1)

    def as_row(column):
        return jnp.sum(jnp.where(tok_rows == tok_lanes, column, 0.0), axis=0, keepdims=True)

    def as_column(row):
        return jnp.sum(jnp.where(tok_rows == tok_lanes, row, 0.0), axis=1, keepdims=True)

    wide = tokens[...].astype(F32)
    squares[t] = jnp.broadcast_to(as_row(jnp.sum(wide * wide, axis=1, keepdims=True)), (8, tok))

    def square_copy(step):
        return copy(squares.at[t], squares.at[t], sq.at[step], rq.at[t], "tensor", at(t, step, n_t))

    pl.semaphore_wait(barrier, n_dp + n_ex + n_t - 3)
    for step in range(1, n_t):
        square_copy(step).start()

    wide_ex = max(128, n_ex)
    ex_rows = lax.broadcasted_iota(jnp.int32, (wide_ex, tok), 0).astype(F32)
    named_t = ex_rows < 0.0
    for k in range(top):
        named_t = named_t | (ex_rows == as_row(ids[:, k : k + 1].astype(F32)))
    count_t = dot(named_t.astype(F32).astype(BF16), (tok_rows < tok_lanes).astype(F32).astype(BF16))
    slot_t[...] = jnp.where(named_t, count_t, -1.0)
    slot_rows = lax.broadcasted_iota(jnp.int32, (cap, tok), 0).astype(F32)

    for step in range(1, n_t):
        s = at(t, step, n_t)
        copy(squares.at[s], squares.at[s], sq.at[step], rq.at[s], "tensor", s).wait_recv()
    total_row = squares[0, 0:1, :]
    for s in range(1, n_t):
        total_row = total_row + squares[s, 0:1, :]
    scale = as_column(lax.rsqrt(total_row / width_all + 1e-06))
    normed[...] = (tokens[...].astype(F32) * scale).astype(BF16)

    def picked(expert):
        pick = (slot_rows == slot_t[pl.ds(expert, 1), :]).astype(F32).astype(BF16)
        return dot(pick, normed[...]).astype(BF16)

    def block(ref, lead, expert):
        if group == 1:
            return ref.at[lead, expert]
        return ref.at[lead, expert // group, pl.ds(pl.multiple_of(lax.rem(expert, group) * cap, cap), cap)]

    def send_z(expert):
        return copy(outgoing.at[expert], block(rows_in, 0, e), sz.at[expert], rz.at[e], "expert", expert)

    def wait_z(source):
        return copy(outgoing.at[source], block(rows_in, 0, source), sz.at[source], rz.at[source], "expert", source)

    def forward_x(src, expert, hop):
        return copy(
            src, block(rows_in, n_dp - hop, expert),
            sx.at[hop, expert], rx.at[n_dp - hop, expert], "dp", at(d, hop, n_dp),
        )

    def wait_x(expert, h):
        return copy(
            block(rows_in, 0, expert), block(rows_in, h, expert),
            sx.at[h, expert], rx.at[h, expert], "dp", at(d, h, n_dp),
        )

    outgoing[e] = picked(e)
    own = pltpu.make_async_copy(outgoing.at[e], block(rows_in, 0, e), w_sem.at[2])
    own.start()
    for hop in range(1, n_dp):
        forward_x(outgoing.at[e], e, hop).start()

    @pl.loop(1, n_ex)
    def _(step):
        expert = at(e, step, n_ex)
        outgoing[expert] = picked(expert)
        send_z(expert).start()

    ex_lanes = lax.broadcasted_iota(jnp.int32, (tok, wide_ex), 1)
    named = ex_lanes == ids[:, 0:1]
    for k in range(1, top):
        named = named | (ex_lanes == ids[:, k : k + 1])
    counts = dot((tok_lanes < tok_rows).astype(F32).astype(BF16), named.astype(F32).astype(BF16))
    lanes = lax.broadcasted_iota(jnp.int32, (tok, n_ex * cap), 1).astype(F32)
    weights = jnp.zeros((tok, n_ex * cap), F32)
    for k in range(top):
        this = ids[:, k : k + 1]
        slot = jnp.sum(jnp.where(ex_lanes == this, counts, 0.0), axis=1, keepdims=True)
        target = this.astype(F32) * cap + slot
        weights = weights + jnp.where(lanes == target, scores[:, k : k + 1].astype(F32), 0.0)
    combine[...] = weights.astype(BF16)

    own.wait()
    load_in.wait()
    load_out.wait()

    def part_copy(h, c, step):
        to = at(t, step, n_t)
        return copy(part.at[h, c, to], part_in.at[h, c, t], sp.at[h, c, step], rp.at[h, c, t], "tensor", to)

    def hidden_copy(h, c, step):
        to = at(t, step, n_t)
        return copy(hidden.at[h, c, t], hidden.at[h, c, t], sh.at[h, c, step], rh.at[h, c, t], "tensor", to)

    def down_copy(h, c):
        return copy(down.at[h, c], down_in.at[n_dp - h, c], so.at[h, c], ro.at[n_dp - h, c], "dp", at(d, h, n_dp))

    def project(h, c):
        @pl.when(h == 0)
        def _():
            for i in range(group):
                source = c * group + i

                @pl.when(source != e)
                def _():
                    wait_z(source).wait_recv()
                    for hop in range(1, n_dp):
                        forward_x(block(rows_in, 0, source), source, hop).start()

        @pl.when(h > 0)
        def _():
            for i in range(group):
                wait_x(c * group + i, h).wait_recv()

        rows = rows_in[h, c]
        for g in range(2):
            sums = dot(rows, w_in[g]).astype(BF16)
            for to in range(n_t):
                part[h, c, to, :, g * sub : (g + 1) * sub] = sums[:, to * sub : (to + 1) * sub]
        for step in range(1, n_t):
            part_copy(h, c, step).start()

    def activate(h, c):
        total = part[h, c, t].astype(F32)
        for step in range(1, n_t):
            s = at(t, step, n_t)
            copy(part.at[h, c, s], part_in.at[h, c, s], sp.at[h, c, step], rp.at[h, c, s], "tensor", s).wait_recv()
            total = total + part_in[h, c, s].astype(F32)
        gate, up = total[:, :sub], total[:, sub:]
        hidden[h, c, t] = (gate / (1.0 + jnp.exp(-gate)) * up).astype(BF16)
        for step in range(1, n_t):
            hidden_copy(h, c, step).start()

    def expand(h, c):
        for step in range(1, n_t):
            s = at(t, step, n_t)
            copy(hidden.at[h, c, s], hidden.at[h, c, s], sh.at[h, c, step], rh.at[h, c, s], "tensor", s).wait_recv()
        full = jnp.concatenate([hidden[h, c, s] for s in range(n_t)], axis=1)
        result = dot(full, w_out[...])

        @pl.when(h == 0)
        def _():
            keep[c] = result

        @pl.when(h > 0)
        def _():
            down[h, c] = result.astype(BF16)

            @pl.when(c != ec)
            def _():
                down_copy(h, c).start()

    def item(number):
        return lax.rem(number, n_dp), at(ec, -(number // n_dp), n_t)

    items = n_dp * n_t

    @pl.loop(0, items + 2)
    def _(step):
        @pl.when(step < items)
        def _():
            project(*item(step))

        @pl.when((step > 0) & (step <= items))
        def _():
            activate(*item(step - 1))

        @pl.when(step > 1)
        def _():
            expand(*item(step - 2))

    for h in range(1, n_dp):
        down_copy(h, ec).start()

    def home_copy(expert):
        return copy(block(home, 0, expert), home_in.at[e], sr.at[expert], rr.at[e], "expert", expert)

    @pl.loop(0, n_t)
    def _(step):
        q = at(ec, -1 - step, n_t)
        total = keep[q]
        for h in range(1, n_dp):
            copy(down.at[h, q], down_in.at[h, q], so.at[h, q], ro.at[h, q], "dp", at(d, h, n_dp)).wait_recv()
            total = total + down_in[h, q].astype(F32)
        home[0, q] = total.astype(BF16)
        for i in range(group):
            expert = q * group + i

            @pl.when(expert != e)
            def _():
                home_copy(expert).start()

            @pl.when(expert == e)
            def _():
                home_in[expert] = home[0, q, i * cap : (i + 1) * cap, :]

    @pl.loop(1, n_ex)
    def _(step):
        source = at(e, step, n_ex)
        copy(block(home, 0, source), home_in.at[source], sr.at[source], rr.at[source], "expert", source).wait_recv()

    mixed[...] = dot(combine[...], home_in[...].reshape(n_ex * cap, width)).astype(BF16)

    @pl.loop(1, n_ex)
    def _(step):
        expert = at(e, step, n_ex)
        send_z(expert).wait_send()
        home_copy(expert).wait_send()

    @pl.loop(0, n_ex)
    def _(expert):
        for hop in range(1, n_dp):
            forward_x(block(rows_in, 0, expert), expert, hop).wait_send()

    for step in range(1, n_t):
        square_copy(step).wait_send()

    @pl.loop(0, n_t)
    def _(c):
        for h in range(n_dp):
            for step in range(1, n_t):
                part_copy(h, c, step).wait_send()
                hidden_copy(h, c, step).wait_send()
        for h in range(1, n_dp):
            down_copy(h, c).wait_send()


def per_device(sizes, tokens, expert_ids, gate_scores, weight_in, weight_out):
    n_dp, n_ex, n_t, cap = sizes
    tok, width = tokens.shape
    units = weight_out.shape[1]
    chunk = n_ex // n_t * cap
    dma = pltpu.SemaphoreType.DMA
    vmem = pl.BlockSpec(memory_space=pltpu.VMEM)
    return pl.pallas_call(
        functools.partial(kernel, sizes),
        out_shape=jax.ShapeDtypeStruct((tok, width), BF16),
        in_specs=[vmem] * 3 + [pl.BlockSpec(memory_space=pl.ANY)] * 2,
        out_specs=vmem,
        scratch_shapes=[
            pltpu.VMEM((2, width, units), BF16),
            pltpu.VMEM((units, width), BF16),
            pltpu.VMEM((n_t, 8, tok), F32),
            pltpu.VMEM((tok, width), BF16),
            pltpu.VMEM((max(128, n_ex), tok), F32),
            pltpu.VMEM((tok, n_ex * cap), BF16),
            pltpu.VMEM((n_ex, cap, width), BF16),
            pltpu.VMEM((n_dp, n_t, chunk, width), BF16),
            pltpu.VMEM((n_dp, n_t, n_t, chunk, 2 * units // n_t), BF16),
            pltpu.VMEM((n_dp, n_t, n_t, chunk, 2 * units // n_t), BF16),
            pltpu.VMEM((n_dp, n_t, n_t, chunk, units // n_t), BF16),
            pltpu.VMEM((n_t, chunk, width), F32),
            pltpu.VMEM((n_dp, n_t, chunk, width), BF16),
            pltpu.VMEM((n_dp, n_t, chunk, width), BF16),
            pltpu.VMEM((1, n_t, chunk, width), BF16),
            pltpu.VMEM((n_ex, cap, width), BF16),
            dma((3,)),
            dma((n_t,)),
            dma((n_t,)),
            dma((n_ex,)),
            dma((n_ex,)),
            dma((n_dp, n_ex)),
            dma((n_dp, n_ex)),
            dma((n_dp, n_t, n_t)),
            dma((n_dp, n_t, n_t)),
            dma((n_dp, n_t, n_t)),
            dma((n_dp, n_t, n_t)),
            dma((n_dp, n_t)),
            dma((n_dp, n_t)),
            dma((n_ex,)),
            dma((n_ex,)),
        ],
        compiler_params=pltpu.CompilerParams(
            collective_id=0, has_side_effects=True, vmem_limit_bytes=60 * 1024 * 1024
        ),
    )(tokens, expert_ids, gate_scores, weight_in, weight_out)


def solution(mesh):
    n_dp, n_ex, n_t = mesh.shape["dp"], mesh.shape["expert"], mesh.shape["tensor"]

    def whole(tokens, expert_ids, gate_scores, weight_in, weight_out):
        tok = tokens.shape[0] // (n_dp * n_ex)
        slots = min(3 * tok * expert_ids.shape[1] // (2 * n_ex), tok)
        cap = -(-slots // 16) * 16
        return jax.shard_map(
            functools.partial(per_device, (n_dp, n_ex, n_t, cap)),
            mesh=mesh,
            in_specs=(
                P(("dp", "expert"), "tensor"),
                P(("dp", "expert"), None),
                P(("dp", "expert"), None),
                P("expert", None, "tensor", "dp"),
                P("expert", "dp", "tensor"),
            ),
            out_specs=P(("dp", "expert"), "tensor"),
            check_vma=False,
        )(tokens, expert_ids, gate_scores, weight_in, weight_out)

    return whole
```

```python
import functools

import jax
import jax.numpy as jnp
from jax import lax
from jax.experimental import pallas as pl
from jax.experimental.pallas import tpu as pltpu
from jax.sharding import PartitionSpec as P

MESH = pl.DeviceIdType.MESH
F32 = jnp.float32
BF16 = jnp.bfloat16


def dot(a, b):
    return jnp.dot(a, b, preferred_element_type=F32)


def kernel(
    sizes,
    tokens,
    ids,
    scores,
    w_in_hbm,
    w_out_hbm,
    mixed,
    w_in,
    w_out,
    squares,
    normed,
    slot_t,
    combine,
    outgoing,
    rows_in,
    part,
    part_in,
    hidden,
    keep,
    down,
    down_in,
    home,
    home_in,
    w_sem,
    sq,
    rq,
    sz,
    rz,
    sx,
    rx,
    sp,
    rp,
    sh,
    rh,
    so,
    ro,
    sr,
    rr,
):
    n_dp, n_ex, n_t, cap = sizes
    d, e, t = lax.axis_index("dp"), lax.axis_index("expert"), lax.axis_index("tensor")
    group = n_ex // n_t
    ec = e // group
    tok, width = tokens.shape
    top = ids.shape[1]
    units = w_out.shape[0]
    sub = units // n_t
    width_all = width * n_t

    def at(index, step, count):
        return lax.rem(index + step + count, count)

    def copy(src, dst, send, recv, axis, index):
        return pltpu.make_async_remote_copy(
            src_ref=src, dst_ref=dst, send_sem=send, recv_sem=recv,
            device_id={axis: index}, device_id_type=MESH,
        )

    barrier = pltpu.get_barrier_semaphore()
    for axis, me, count in (("dp", d, n_dp), ("expert", e, n_ex), ("tensor", t, n_t)):
        for step in range(1, count):
            pl.semaphore_signal(
                barrier, inc=1, device_id={axis: at(me, step, count)}, device_id_type=MESH
            )
    load_in = pltpu.make_async_copy(w_in_hbm.at[0], w_in, w_sem.at[0])
    load_out = pltpu.make_async_copy(w_out_hbm.at[0], w_out, w_sem.at[1])
    load_in.start()
    load_out.start()

    tok_rows = lax.broadcasted_iota(jnp.int32, (tok, tok), 0)
    tok_lanes = lax.broadcasted_iota(jnp.int32, (tok, tok), 1)

    def as_row(column):
        return jnp.sum(jnp.where(tok_rows == tok_lanes, column, 0.0), axis=0, keepdims=True)

    def as_column(row):
        return jnp.sum(jnp.where(tok_rows == tok_lanes, row, 0.0), axis=1, keepdims=True)

    wide = tokens[...].astype(F32)
    squares[t] = jnp.broadcast_to(as_row(jnp.sum(wide * wide, axis=1, keepdims=True)), (8, tok))

    def square_copy(step):
        return copy(squares.at[t], squares.at[t], sq.at[step], rq.at[t], "tensor", at(t, step, n_t))

    pl.semaphore_wait(barrier, n_dp + n_ex + n_t - 3)
    for step in range(1, n_t):
        square_copy(step).start()

    wide_ex = max(128, n_ex)
    ex_rows = lax.broadcasted_iota(jnp.int32, (wide_ex, tok), 0).astype(F32)
    named_t = ex_rows < 0.0
    for k in range(top):
        named_t = named_t | (ex_rows == as_row(ids[:, k : k + 1].astype(F32)))
    count_t = dot(named_t.astype(F32).astype(BF16), (tok_rows < tok_lanes).astype(F32).astype(BF16))
    slot_t[...] = jnp.where(named_t, count_t, -1.0)
    slot_rows = lax.broadcasted_iota(jnp.int32, (cap, tok), 0).astype(F32)

    for step in range(1, n_t):
        s = at(t, step, n_t)
        copy(squares.at[s], squares.at[s], sq.at[step], rq.at[s], "tensor", s).wait_recv()
    total_row = squares[0, 0:1, :]
    for s in range(1, n_t):
        total_row = total_row + squares[s, 0:1, :]
    scale = as_column(lax.rsqrt(total_row / width_all + 1e-06))
    normed[...] = (tokens[...].astype(F32) * scale).astype(BF16)

    def picked(expert):
        pick = (slot_rows == slot_t[pl.ds(expert, 1), :]).astype(F32).astype(BF16)
        return dot(pick, normed[...]).astype(BF16)

    def block(ref, lead, expert):
        if group == 1:
            return ref.at[lead, expert]
        return ref.at[lead, expert // group, pl.ds(pl.multiple_of(lax.rem(expert, group) * cap, cap), cap)]

    def send_z(expert):
        return copy(outgoing.at[expert], block(rows_in, 0, e), sz.at[expert], rz.at[e], "expert", expert)

    def wait_z(source):
        return copy(outgoing.at[source], block(rows_in, 0, source), sz.at[source], rz.at[source], "expert", source)

    def forward_x(src, expert, hop):
        return copy(
            src, block(rows_in, n_dp - hop, expert),
            sx.at[hop, expert], rx.at[n_dp - hop, expert], "dp", at(d, hop, n_dp),
        )

    def wait_x(expert, h):
        return copy(
            block(rows_in, 0, expert), block(rows_in, h, expert),
            sx.at[h, expert], rx.at[h, expert], "dp", at(d, h, n_dp),
        )

    outgoing[e] = picked(e)
    own = pltpu.make_async_copy(outgoing.at[e], block(rows_in, 0, e), w_sem.at[2])
    own.start()
    for hop in range(1, n_dp):
        forward_x(outgoing.at[e], e, hop).start()

    @pl.loop(1, n_ex)
    def _(step):
        expert = at(e, step, n_ex)
        outgoing[expert] = picked(expert)
        send_z(expert).start()

    ex_lanes = lax.broadcasted_iota(jnp.int32, (tok, wide_ex), 1)
    named = ex_lanes == ids[:, 0:1]
    for k in range(1, top):
        named = named | (ex_lanes == ids[:, k : k + 1])
    counts = dot((tok_lanes < tok_rows).astype(F32).astype(BF16), named.astype(F32).astype(BF16))
    lanes = lax.broadcasted_iota(jnp.int32, (tok, n_ex * cap), 1).astype(F32)
    weights = jnp.zeros((tok, n_ex * cap), F32)
    for k in range(top):
        this = ids[:, k : k + 1]
        slot = jnp.sum(jnp.where(ex_lanes == this, counts, 0.0), axis=1, keepdims=True)
        target = this.astype(F32) * cap + slot
        weights = weights + jnp.where(lanes == target, scores[:, k : k + 1].astype(F32), 0.0)
    combine[...] = weights.astype(BF16)

    own.wait()
    load_in.wait()
    load_out.wait()

    def part_copy(h, c, step):
        to = at(t, step, n_t)
        return copy(part.at[h, c, to], part_in.at[h, c, t], sp.at[h, c, step], rp.at[h, c, t], "tensor", to)

    def hidden_copy(h, c, step):
        to = at(t, step, n_t)
        return copy(hidden.at[h, c, t], hidden.at[h, c, t], sh.at[h, c, step], rh.at[h, c, t], "tensor", to)

    def down_copy(h, c):
        return copy(down.at[h, c], down_in.at[n_dp - h, c], so.at[h, c], ro.at[n_dp - h, c], "dp", at(d, h, n_dp))

    def project(h, c):
        @pl.when(h == 0)
        def _():
            for i in range(group):
                source = c * group + i

                @pl.when(source != e)
                def _():
                    wait_z(source).wait_recv()
                    for hop in range(1, n_dp):
                        forward_x(block(rows_in, 0, source), source, hop).start()

        @pl.when(h > 0)
        def _():
            for i in range(group):
                wait_x(c * group + i, h).wait_recv()

        rows = rows_in[h, c]
        for g in range(2):
            sums = dot(rows, w_in[g]).astype(BF16)
            for to in range(n_t):
                part[h, c, to, :, g * sub : (g + 1) * sub] = sums[:, to * sub : (to + 1) * sub]
        for step in range(1, n_t):
            part_copy(h, c, step).start()

    def activate(h, c):
        total = part[h, c, t].astype(F32)
        for step in range(1, n_t):
            s = at(t, step, n_t)
            copy(part.at[h, c, s], part_in.at[h, c, s], sp.at[h, c, step], rp.at[h, c, s], "tensor", s).wait_recv()
            total = total + part_in[h, c, s].astype(F32)
        gate, up = total[:, :sub], total[:, sub:]
        hidden[h, c, t] = (gate / (1.0 + jnp.exp(-gate)) * up).astype(BF16)
        for step in range(1, n_t):
            hidden_copy(h, c, step).start()

    def expand(h, c):
        for step in range(1, n_t):
            s = at(t, step, n_t)
            copy(hidden.at[h, c, s], hidden.at[h, c, s], sh.at[h, c, step], rh.at[h, c, s], "tensor", s).wait_recv()
        full = jnp.concatenate([hidden[h, c, s] for s in range(n_t)], axis=1)
        result = dot(full, w_out[...])

        @pl.when(h == 0)
        def _():
            keep[c] = result

        @pl.when(h > 0)
        def _():
            down[h, c] = result.astype(BF16)

            @pl.when(c != ec)
            def _():
                down_copy(h, c).start()

            @pl.when((c == at(ec, 1, n_t)) & (h == n_dp - 1))
            def _():
                for far in range(1, n_dp):
                    down_copy(far, ec).start()

    def home_copy(expert):
        return copy(block(home, 0, expert), home_in.at[e], sr.at[expert], rr.at[e], "expert", expert)

    def collect(step):
        q = at(ec, -1 - step, n_t)
        total = keep[q]
        for h in range(1, n_dp):
            copy(down.at[h, q], down_in.at[h, q], so.at[h, q], ro.at[h, q], "dp", at(d, h, n_dp)).wait_recv()
            total = total + down_in[h, q].astype(F32)
        home[0, q] = total.astype(BF16)
        for i in range(group):
            expert = q * group + i

            @pl.when(expert != e)
            def _():
                home_copy(expert).start()

            @pl.when(expert == e)
            def _():
                home_in[expert] = home[0, q, i * cap : (i + 1) * cap, :]

    def item(number):
        return lax.rem(number, n_dp), at(ec, -(number // n_dp), n_t)

    items = n_dp * n_t

    @pl.loop(0, items + 2 + 1)
    def _(step):
        @pl.when(step < items)
        def _():
            project(*item(step))

        @pl.when((step > 0) & (step <= items))
        def _():
            activate(*item(step - 1))

        @pl.when((step > 1) & (step < items + 2))
        def _():
            expand(*item(step - 2))

        for k in range(1, n_t):

            @pl.when(step == (k + 1) * n_dp + 2)
            def _():
                collect(k - 1)

    collect(n_t - 1)

    @pl.loop(1, n_ex)
    def _(step):
        source = at(e, step, n_ex)
        copy(block(home, 0, source), home_in.at[source], sr.at[source], rr.at[source], "expert", source).wait_recv()

    mixed[...] = dot(combine[...], home_in[...].reshape(n_ex * cap, width)).astype(BF16)

    @pl.loop(1, n_ex)
    def _(step):
        expert = at(e, step, n_ex)
        send_z(expert).wait_send()
        home_copy(expert).wait_send()

    @pl.loop(0, n_ex)
    def _(expert):
        for hop in range(1, n_dp):
            forward_x(block(rows_in, 0, expert), expert, hop).wait_send()

    for step in range(1, n_t):
        square_copy(step).wait_send()

    @pl.loop(0, n_t)
    def _(c):
        for h in range(n_dp):
            for step in range(1, n_t):
                part_copy(h, c, step).wait_send()
                hidden_copy(h, c, step).wait_send()
        for h in range(1, n_dp):
            down_copy(h, c).wait_send()


def per_device(sizes, tokens, expert_ids, gate_scores, weight_in, weight_out):
    n_dp, n_ex, n_t, cap = sizes
    tok, width = tokens.shape
    units = weight_out.shape[1]
    chunk = n_ex // n_t * cap
    dma = pltpu.SemaphoreType.DMA
    vmem = pl.BlockSpec(memory_space=pltpu.VMEM)
    return pl.pallas_call(
        functools.partial(kernel, sizes),
        out_shape=jax.ShapeDtypeStruct((tok, width), BF16),
        in_specs=[vmem] * 3 + [pl.BlockSpec(memory_space=pl.ANY)] * 2,
        out_specs=vmem,
        scratch_shapes=[
            pltpu.VMEM((2, width, units), BF16),
            pltpu.VMEM((units, width), BF16),
            pltpu.VMEM((n_t, 8, tok), F32),
            pltpu.VMEM((tok, width), BF16),
            pltpu.VMEM((max(128, n_ex), tok), F32),
            pltpu.VMEM((tok, n_ex * cap), BF16),
            pltpu.VMEM((n_ex, cap, width), BF16),
            pltpu.VMEM((n_dp, n_t, chunk, width), BF16),
            pltpu.VMEM((n_dp, n_t, n_t, chunk, 2 * units // n_t), BF16),
            pltpu.VMEM((n_dp, n_t, n_t, chunk, 2 * units // n_t), BF16),
            pltpu.VMEM((n_dp, n_t, n_t, chunk, units // n_t), BF16),
            pltpu.VMEM((n_t, chunk, width), F32),
            pltpu.VMEM((n_dp, n_t, chunk, width), BF16),
            pltpu.VMEM((n_dp, n_t, chunk, width), BF16),
            pltpu.VMEM((1, n_t, chunk, width), BF16),
            pltpu.VMEM((n_ex, cap, width), BF16),
            dma((3,)),
            dma((n_t,)),
            dma((n_t,)),
            dma((n_ex,)),
            dma((n_ex,)),
            dma((n_dp, n_ex)),
            dma((n_dp, n_ex)),
            dma((n_dp, n_t, n_t)),
            dma((n_dp, n_t, n_t)),
            dma((n_dp, n_t, n_t)),
            dma((n_dp, n_t, n_t)),
            dma((n_dp, n_t)),
            dma((n_dp, n_t)),
            dma((n_ex,)),
            dma((n_ex,)),
        ],
        compiler_params=pltpu.CompilerParams(
            collective_id=0, has_side_effects=True, vmem_limit_bytes=60 * 1024 * 1024
        ),
    )(tokens, expert_ids, gate_scores, weight_in, weight_out)


def solution(mesh):
    n_dp, n_ex, n_t = mesh.shape["dp"], mesh.shape["expert"], mesh.shape["tensor"]

    def whole(tokens, expert_ids, gate_scores, weight_in, weight_out):
        tok = tokens.shape[0] // (n_dp * n_ex)
        slots = min(3 * tok * expert_ids.shape[1] // (2 * n_ex), tok)
        cap = -(-slots // 16) * 16
        return jax.shard_map(
            functools.partial(per_device, (n_dp, n_ex, n_t, cap)),
            mesh=mesh,
            in_specs=(
                P(("dp", "expert"), "tensor"),
                P(("dp", "expert"), None),
                P(("dp", "expert"), None),
                P("expert", None, "tensor", "dp"),
                P("expert", "dp", "tensor"),
            ),
            out_specs=P(("dp", "expert"), "tensor"),
            check_vma=False,
        )(tokens, expert_ids, gate_scores, weight_in, weight_out)

    return whole
```
